32 devices in a mesh: row: 8 (over y, x, core), col: 4 (over z).
Axes of the slice: x: 2, y: 2, z: 4, core: 2. Of those that a mesh axis runs over, the one named last changes fastest.
Arguments:
- jacobian: float32 [2, 4096, 256], P(None, ('row', 'col')), may hold values from -0.25 to 0.25
Outputs:
- normal_tiles: float32 [8, 2, 4, 512, 512], P('row', None, 'col')
The draws below stay inside these ranges and needn't reach their ends.
All inputs are finite; a program needn't handle non-finite values.
Results may differ from the reference program's by a relative error of at most 0.0003.
Values sent between devices are 32-bit elements; how exact they have to be, the bound alone decides.
A program may use at most 64 MiB of HBM per device.

```python
import jax
import jax.numpy as jnp
from jax import lax

TILE = 512
KP = 256
PANELS = 2
NT = 8
CYC = 2
M = 4096
N_COL = 4


def block_levels(stream_key, shape, shards, smallest, largest):
    factor_of, own = 1.0, jax.random.fold_in(stream_key, 6)
    for dim, shards_of in shards:
        heights = jnp.exp(jax.random.uniform(jax.random.fold_in(own, dim), (shards_of,), jnp.float32, smallest / len(shards), largest / len(shards)))
        factor_of = factor_of * jnp.repeat(heights, shape[dim] // shards_of).reshape([-1 if axis == dim else 1 for axis in range(len(shape))])
    return factor_of


def gaussian(stream_key, dims, width, limit, pieces=(), kind=jnp.bfloat16):
    result = jax.random.normal(stream_key, dims, jnp.float32) * width
    if len(pieces) > 0:
        result = block_levels(stream_key, dims, pieces, -0.22, 0.18) * result
    return jnp.clip(result, min=-limit, max=limit).astype(kind)


def setup_inputs(seed: int = 0) -> dict:
    streams_of = jax.random.split(jax.random.key(seed), 2)
    jacobian = gaussian(streams_of[0], (PANELS, M, KP), (PANELS * KP) ** -0.5, 0.25, ((1, 32),), jnp.float32)
    return {"jacobian": jacobian}


def reference(jacobian):
    def one_row(index):
        row_block = lax.dynamic_slice_in_dim(jacobian, index * TILE, TILE, 1)
        products = jnp.einsum("pak,pbk->ab", row_block.astype(jnp.float32), jacobian.astype(jnp.float32), precision=lax.Precision.HIGHEST)
        arranged = products.reshape(TILE, CYC, N_COL, TILE).transpose(1, 2, 0, 3)
        column_tile = jnp.arange(CYC, dtype=jnp.int32)[:, None] * N_COL + jnp.arange(N_COL, dtype=jnp.int32)[None, :]
        keep_mask = column_tile <= index
        return jnp.where(keep_mask[:, :, None, None], arranged, jnp.zeros_like(arranged))
    return lax.map(one_row, jnp.arange(NT, dtype=jnp.int32))
```

```python
import functools

import jax
import jax.numpy as jnp
from jax import lax
from jax.experimental import pallas as pl
from jax.experimental.pallas import tpu as pltpu
from jax.sharding import PartitionSpec as P

SPLIT = 1
MESH = pl.DeviceIdType.MESH


def flip(index, bit):
    size = 1 << bit
    return index + (1 - 2 * (index // size % 2)) * size


def kernel(row_count, col_count, x_hbm, out, own, cols, left, right,
           in_sem, z_send, z_recv, c_send, c_recv, barrier_go):
    row = lax.axis_index("row")
    col = lax.axis_index("col")
    turns = row_count // col_count
    panels, height, width = own.shape[1:]
    piece = height // SPLIT
    pieces = [(p, pl.ds(h * piece, piece)) for p in range(panels) for h in range(SPLIT)]
    bits = (row_count // 2).bit_length() - 1
    parity = row % 2
    sibling = flip(row, 0)
    sign = 2 * parity - 1
    carrier = parity == col % 2

    load = pltpu.make_async_copy(x_hbm, own.at[col], in_sem)
    load.start()

    barrier = pltpu.get_barrier_semaphore()

    def greet(r, c):
        pl.semaphore_signal(barrier, inc=1, device_id={"row": r, "col": c}, device_id_type=MESH)

    for bit in range(bits + 1):
        greet(flip(row, bit), col)

    @pl.when(col > 0)
    def _():
        greet(row, col - 1)

    @pl.when(col < col_count - 1)
    def _():
        greet(row, col + 1)

    peers = bits + 1 + (col > 0).astype(jnp.int32) + (col < col_count - 1).astype(jnp.int32)
    pl.semaphore_wait(barrier, peers)
    load.wait()

    def along(phase):
        return sign if phase == 0 else -sign

    def line_copy(phase, step, k):
        to = col + along(phase)
        origin = col - along(phase) * step
        part = own.at[origin, pieces[k][0], pieces[k][1]]
        return pltpu.make_async_remote_copy(
            src_ref=part, dst_ref=part,
            send_sem=z_send.at[phase, step, k], recv_sem=z_recv.at[origin, k],
            device_id={"row": row, "col": to}, device_id_type=MESH)

    def origin_ok(phase, step):
        origin = col - along(phase) * step
        return (origin >= 0) & (origin < col_count)

    def target_ok(phase):
        to = col + along(phase)
        return (to >= 0) & (to < col_count)

    def tile_copy(turn, origin, k, bit, from_own):
        where = (pieces[k][0], pieces[k][1])
        landing = cols.at[(turn, origin) + where]
        source = own.at[(origin,) + where] if from_own else landing
        return pltpu.make_async_remote_copy(
            src_ref=source, dst_ref=landing,
            send_sem=c_send.at[turn, origin, k, bit], recv_sem=c_recv.at[turn, origin, k],
            device_id={"row": flip(row, bit), "col": col}, device_id_type=MESH)

    def distance(turn):
        home = (col + col_count * turn) // 2
        chip = row // 2
        d = 0
        for bit in range(bits):
            low = chip // (1 << bit) % 2
            far = home // (1 << bit) % 2
            d = d + (low + far) % 2 * (1 << bit)
        return d

    distances = [distance(turn) for turn in range(turns)]
    at_home = row % col_count == col
    home_turn = row // col_count
    away = [row != col + col_count * turn for turn in range(turns)]

    def spread(turn, origin, k):
        for bit in reversed(range(bits)):
            @pl.when(distances[turn] < (1 << bit))
            def _(bit=bit):
                tile_copy(turn, origin, k, bit + 1, False).start()
        tile_copy(turn, origin, k, 0, False).start()

    def line_step(phase, step):
        @pl.when(origin_ok(phase, step))
        def _():
            origin = col - along(phase) * step
            for k in range(len(pieces)):
                if step > 0:
                    line_copy(phase, step, k).wait_recv()

                @pl.when(target_ok(phase))
                def _(k=k):
                    line_copy(phase, step, k).start()

                if phase == 0 or step > 0:
                    @pl.when(at_home)
                    def _(k=k):
                        for bit in reversed(range(bits + 1)):
                            tile_copy(home_turn, origin, k, bit, True).start()

    def tile_step(phase, step):
        @pl.when(origin_ok(phase, step) & carrier)
        def _():
            origin = col - along(phase) * step
            for k in range(len(pieces)):
                for turn in range(turns):
                    @pl.when(away[turn])
                    def _(turn=turn, k=k):
                        tile_copy(turn, origin, k, 0, False).wait_recv()
                        spread(turn, origin, k)

    def line_drain(phase):
        @pl.when(target_ok(phase))
        def _():
            for step in range(col_count):
                @pl.when(origin_ok(phase, step))
                def _(step=step):
                    for k in range(len(pieces)):
                        line_copy(phase, step, k).wait_send()

    def swap():
        line_drain(0)
        pl.semaphore_signal(barrier_go, inc=1, device_id={"row": sibling, "col": col},
                            device_id_type=MESH)
        pl.semaphore_wait(barrier_go, 1)

    steps = [(0, step) for step in range(col_count)] + [(1, step) for step in range(col_count)]
    behind = []
    for phase, step in steps:
        if phase == 1 and step == 0:
            swap()
        line_step(phase, step)
        if len(behind) > 0:
            tile_step(*behind.pop(0))
        if phase == 0 or step > 0:
            behind.append((phase, step))
    for item in behind:
        tile_step(*item)

    line_drain(1)

    def each_origin(origin, carry):
        for turn in range(turns):
            for k in range(len(pieces)):
                @pl.when(carrier)
                def _(turn=turn, k=k):
                    for bit in range(bits):
                        @pl.when(distances[turn] < (1 << bit))
                        def _(bit=bit):
                            tile_copy(turn, origin, k, bit + 1, False).wait_send()
                    tile_copy(turn, origin, k, 0, False).wait_send()

                @pl.when(jnp.logical_not(carrier))
                def _(turn=turn, k=k):
                    tile_copy(turn, origin, k, 0, False).wait_recv()
        return carry

    lax.fori_loop(0, col_count, each_origin, 0)

    depth = panels * width

    def fill(target, block, places):
        for origin in range(col_count):
            for p in range(panels):
                value = block[origin, p]
                high = value.astype(jnp.bfloat16)
                low = (value - high.astype(jnp.float32)).astype(jnp.bfloat16)
                for place, half in enumerate(places):
                    target[pl.ds(origin * height, height), pl.ds(place * depth + p * width, width)] = (
                        high if half == 0 else low)

    fill(left, own, (0, 0, 1))
    for turn in range(turns):
        tile = col + col_count * turn

        @pl.when(tile > row)
        def _(turn=turn):
            out[turn] = jnp.zeros(out.shape[1:], jnp.float32)

        @pl.when(tile <= row)
        def _(turn=turn):
            @pl.when(jnp.logical_not(away[turn]))
            def _():
                fill(right, own, (0, 1, 0))

            @pl.when(away[turn])
            def _():
                fill(right, cols.at[turn], (0, 1, 0))

            out[turn] = lax.dot_general(left[...], right[...], (((1,), (1,)), ((), ())),
                                        preferred_element_type=jnp.float32)


def body(jacobian):
    row_count = lax.axis_size("row")
    col_count = lax.axis_size("col")
    turns = row_count // col_count
    panels, height, width = jacobian.shape
    tile = height * col_count
    pieces = panels * SPLIT
    bits = (row_count // 2).bit_length() - 1
    dma = pltpu.SemaphoreType.DMA
    blocks = pl.pallas_call(
        functools.partial(kernel, row_count, col_count),
        out_shape=jax.ShapeDtypeStruct((turns, tile, tile), jnp.float32),
        in_specs=[pl.BlockSpec(memory_space=pl.ANY)],
        out_specs=pl.BlockSpec(memory_space=pltpu.VMEM),
        scratch_shapes=[
            pltpu.VMEM((col_count, panels, height, width), jnp.float32),
            pltpu.VMEM((turns, col_count, panels, height, width), jnp.float32),
            pltpu.VMEM((tile, 3 * panels * width), jnp.bfloat16),
            pltpu.VMEM((tile, 3 * panels * width), jnp.bfloat16),
            dma,
            dma((2, col_count, pieces)),
            dma((col_count, pieces)),
            dma((turns, col_count, pieces, bits + 1)),
            dma((turns, col_count, pieces)),
            pltpu.SemaphoreType.REGULAR,
        ],
        compiler_params=pltpu.CompilerParams(collective_id=0, has_side_effects=True),
    )(jacobian)
    return blocks[None, :, None]


def solution(mesh):
    in_specs = (P(None, ("row", "col"), None),)
    out_specs = P("row", None, "col", None, None)
    return jax.shard_map(body, mesh=mesh, in_specs=in_specs, out_specs=out_specs, check_vma=False)
```

```python
import functools

import jax
import jax.numpy as jnp
from jax import lax
from jax.experimental import pallas as pl
from jax.experimental.pallas import tpu as pltpu
from jax.sharding import PartitionSpec as P

SPLIT = 2
RELAY_LAG = 1
LEAF_LAG = 2
MESH = pl.DeviceIdType.MESH


def flip(index, bit):
    size = 1 << bit
    return index + (1 - 2 * (index // size % 2)) * size


def kernel(row_count, col_count, x_hbm, out, own, cols, left, right,
           in_sem, z_send, z_recv, c_send, c_recv):
    row = lax.axis_index("row")
    col = lax.axis_index("col")
    turns = row_count // col_count
    panels, height, width = own.shape[1:]
    piece = height // SPLIT
    pieces = [(p, pl.ds(h * piece, piece)) for p in range(panels) for h in range(SPLIT)]
    bits = (row_count // 2).bit_length() - 1
    parity = row % 2
    sign = 2 * parity - 1
    carrier = parity == col % 2

    load = pltpu.make_async_copy(x_hbm, own.at[col], in_sem)
    load.start()

    barrier = pltpu.get_barrier_semaphore()

    def greet(r, c):
        pl.semaphore_signal(barrier, inc=1, device_id={"row": r, "col": c}, device_id_type=MESH)

    for bit in range(bits + 1):
        greet(flip(row, bit), col)

    @pl.when(col > 0)
    def _():
        greet(row, col - 1)

    @pl.when(col < col_count - 1)
    def _():
        greet(row, col + 1)

    peers = bits + 1 + (col > 0).astype(jnp.int32) + (col < col_count - 1).astype(jnp.int32)
    pl.semaphore_wait(barrier, peers)
    load.wait()

    def along(phase):
        return sign if phase == 0 else -sign

    def line_copy(phase, step, k):
        to = col + along(phase)
        origin = col - along(phase) * step
        part = own.at[origin, pieces[k][0], pieces[k][1]]
        return pltpu.make_async_remote_copy(
            src_ref=part, dst_ref=part,
            send_sem=z_send.at[phase, step, k], recv_sem=z_recv.at[origin, k],
            device_id={"row": row, "col": to}, device_id_type=MESH)

    def origin_ok(phase, step):
        origin = col - along(phase) * step
        return (origin >= 0) & (origin < col_count)

    def target_ok(phase):
        to = col + along(phase)
        return (to >= 0) & (to < col_count)

    def tile_copy(turn, origin, k, bit, from_own):
        where = (pieces[k][0], pieces[k][1])
        landing = cols.at[(turn, origin) + where]
        source = own.at[(origin,) + where] if from_own else landing
        return pltpu.make_async_remote_copy(
            src_ref=source, dst_ref=landing,
            send_sem=c_send.at[turn, origin, k, bit], recv_sem=c_recv.at[turn, origin, k],
            device_id={"row": flip(row, bit), "col": col}, device_id_type=MESH)

    def distance(turn):
        home = (col + col_count * turn) // 2
        chip = row // 2
        d = 0
        for bit in range(bits):
            low = chip // (1 << bit) % 2
            far = home // (1 << bit) % 2
            d = d + (low + far) % 2 * (1 << bit)
        return d

    distances = [distance(turn) for turn in range(turns)]
    at_home = row % col_count == col
    home_turn = row // col_count
    away = [row != col + col_count * turn for turn in range(turns)]

    def spread(turn, origin, k):
        for bit in reversed(range(bits)):
            @pl.when(distances[turn] < (1 << bit))
            def _(bit=bit):
                tile_copy(turn, origin, k, bit + 1, False).start()
        tile_copy(turn, origin, k, 0, False).start()

    def line_step(phase, step):
        @pl.when(origin_ok(phase, step))
        def _():
            origin = col - along(phase) * step
            for k in range(len(pieces)):
                if step > 0:
                    line_copy(phase, step, k).wait_recv()

                @pl.when(target_ok(phase))
                def _(k=k):
                    line_copy(phase, step, k).start()

                if phase == 0 or step > 0:
                    @pl.when(at_home)
                    def _(k=k):
                        for bit in reversed(range(bits + 1)):
                            tile_copy(home_turn, origin, k, bit, True).start()

    relays = [carrier & away[turn] & (distances[turn] < (1 << (bits - 1))) for turn in range(turns)]
    leaves = [carrier & (distances[turn] >= (1 << (bits - 1))) for turn in range(turns)]

    def tile_step(phase, step, roles):
        @pl.when(origin_ok(phase, step))
        def _():
            origin = col - along(phase) * step
            for k in range(len(pieces)):
                for turn in range(turns):
                    @pl.when(roles[turn])
                    def _(turn=turn, k=k):
                        tile_copy(turn, origin, k, 0, False).wait_recv()
                        if roles is relays:
                            spread(turn, origin, k)
                        else:
                            tile_copy(turn, origin, k, 0, False).start()

    def line_drain(phase):
        @pl.when(target_ok(phase))
        def _():
            for step in range(col_count):
                @pl.when(origin_ok(phase, step))
                def _(step=step):
                    for k in range(len(pieces)):
                        line_copy(phase, step, k).wait_send()

    steps = [(0, step) for step in range(col_count)] + [(1, step) for step in range(1, col_count)]
    for place in range(len(steps) + LEAF_LAG):
        if place < len(steps):
            line_step(*steps[place])
            if steps[place] == (0, 0):
                line_step(1, 0)
        if 0 <= place - RELAY_LAG < len(steps):
            tile_step(*steps[place - RELAY_LAG], relays)
        if 0 <= place - LEAF_LAG < len(steps):
            tile_step(*steps[place - LEAF_LAG], leaves)

    line_drain(0)
    line_drain(1)

    def each_origin(origin, carry):
        for turn in range(turns):
            for k in range(len(pieces)):
                @pl.when(carrier)
                def _(turn=turn, k=k):
                    for bit in range(bits):
                        @pl.when(distances[turn] < (1 << bit))
                        def _(bit=bit):
                            tile_copy(turn, origin, k, bit + 1, False).wait_send()
                    tile_copy(turn, origin, k, 0, False).wait_send()

                @pl.when(jnp.logical_not(carrier))
                def _(turn=turn, k=k):
                    tile_copy(turn, origin, k, 0, False).wait_recv()
        return carry

    lax.fori_loop(0, col_count, each_origin, 0)

    depth = panels * width

    def fill(target, block, places):
        for origin in range(col_count):
            for p in range(panels):
                value = block[origin, p]
                high = value.astype(jnp.bfloat16)
                low = (value - high.astype(jnp.float32)).astype(jnp.bfloat16)
                for place, half in enumerate(places):
                    target[pl.ds(origin * height, height), pl.ds(place * depth + p * width, width)] = (
                        high if half == 0 else low)

    fill(left, own, (0, 0, 1))
    for turn in range(turns):
        tile = col + col_count * turn

        @pl.when(tile > row)
        def _(turn=turn):
            out[turn] = jnp.zeros(out.shape[1:], jnp.float32)

        @pl.when(tile <= row)
        def _(turn=turn):
            @pl.when(jnp.logical_not(away[turn]))
            def _():
                fill(right, own, (0, 1, 0))

            @pl.when(away[turn])
            def _():
                fill(right, cols.at[turn], (0, 1, 0))

            out[turn] = lax.dot_general(left[...], right[...], (((1,), (1,)), ((), ())),
                                        preferred_element_type=jnp.float32)


def body(jacobian):
    row_count = lax.axis_size("row")
    col_count = lax.axis_size("col")
    turns = row_count // col_count
    panels, height, width = jacobian.shape
    tile = height * col_count
    pieces = panels * SPLIT
    bits = (row_count // 2).bit_length() - 1
    dma = pltpu.SemaphoreType.DMA
    blocks = pl.pallas_call(
        functools.partial(kernel, row_count, col_count),
        out_shape=jax.ShapeDtypeStruct((turns, tile, tile), jnp.float32),
        in_specs=[pl.BlockSpec(memory_space=pl.ANY)],
        out_specs=pl.BlockSpec(memory_space=pltpu.VMEM),
        scratch_shapes=[
            pltpu.VMEM((col_count, panels, height, width), jnp.float32),
            pltpu.VMEM((turns, col_count, panels, height, width), jnp.float32),
            pltpu.VMEM((tile, 3 * panels * width), jnp.bfloat16),
            pltpu.VMEM((tile, 3 * panels * width), jnp.bfloat16),
            dma,
            dma((2, col_count, pieces)),
            dma((col_count, pieces)),
            dma((turns, col_count, pieces, bits + 1)),
            dma((turns, col_count, pieces)),
        ],
        compiler_params=pltpu.CompilerParams(collective_id=0, has_side_effects=True),
    )(jacobian)
    return blocks[None, :, None]


def solution(mesh):
    in_specs = (P(None, ("row", "col"), None),)
    out_specs = P("row", None, "col", None, None)
    return jax.shard_map(body, mesh=mesh, in_specs=in_specs, out_specs=out_specs, check_vma=False)
```

```python
import functools

import jax
import jax.numpy as jnp
from jax import lax
from jax.experimental import pallas as pl
from jax.experimental.pallas import tpu as pltpu
from jax.sharding import PartitionSpec as P

SPLIT = 2
RELAY_LAG = 1
LEAF_LAG = 4
MESH = pl.DeviceIdType.MESH


def flip(index, bit):
    size = 1 << bit
    return index + (1 - 2 * (index // size % 2)) * size


def kernel(row_count, col_count, x_hbm, out, own, cols, left, right,
           in_sem, z_send, z_recv, c_send, c_recv, f_send):
    row = lax.axis_index("row")
    col = lax.axis_index("col")
    turns = row_count // col_count
    panels, height, width = own.shape[1:]
    piece = height // SPLIT
    pieces = [(p, pl.ds(h * piece, piece)) for p in range(panels) for h in range(SPLIT)]
    bits = (row_count // 2).bit_length() - 1
    parity = row % 2
    sign = 2 * parity - 1
    carrier = parity == col % 2

    load = pltpu.make_async_copy(x_hbm, own.at[col], in_sem)
    load.start()

    barrier = pltpu.get_barrier_semaphore()

    def greet(r, c):
        pl.semaphore_signal(barrier, inc=1, device_id={"row": r, "col": c}, device_id_type=MESH)

    for bit in range(bits + 1):
        greet(flip(row, bit), col)

    if bits == 2:
        greet(flip(flip(row, 1), 2), col)

    @pl.when(col > 0)
    def _():
        greet(row, col - 1)

    @pl.when(col < col_count - 1)
    def _():
        greet(row, col + 1)

    peers = bits + 1 + (bits == 2) + (col > 0).astype(jnp.int32) + (col < col_count - 1).astype(jnp.int32)
    pl.semaphore_wait(barrier, peers)
    load.wait()

    def along(phase):
        return sign if phase == 0 else -sign

    def line_copy(phase, step, k):
        to = col + along(phase)
        origin = col - along(phase) * step
        part = own.at[origin, pieces[k][0], pieces[k][1]]
        return pltpu.make_async_remote_copy(
            src_ref=part, dst_ref=part,
            send_sem=z_send.at[phase, step, k], recv_sem=z_recv.at[origin, k],
            device_id={"row": row, "col": to}, device_id_type=MESH)

    def origin_ok(phase, step):
        origin = col - along(phase) * step
        return (origin >= 0) & (origin < col_count)

    def target_ok(phase):
        to = col + along(phase)
        return (to >= 0) & (to < col_count)

    def tile_copy(turn, origin, k, bit, from_own):
        where = (pieces[k][0], pieces[k][1])
        landing = cols.at[(turn, origin) + where]
        source = own.at[(origin,) + where] if from_own else landing
        return pltpu.make_async_remote_copy(
            src_ref=source, dst_ref=landing,
            send_sem=c_send.at[turn, origin, k, bit], recv_sem=c_recv.at[turn, origin, k],
            device_id={"row": flip(row, bit), "col": col}, device_id_type=MESH)

    def distance(turn):
        home = (col + col_count * turn) // 2
        chip = row // 2
        d = 0
        for bit in range(bits):
            low = chip // (1 << bit) % 2
            far = home // (1 << bit) % 2
            d = d + (low + far) % 2 * (1 << bit)
        return d

    distances = [distance(turn) for turn in range(turns)]
    at_home = row % col_count == col
    home_turn = row // col_count
    away = [row != col + col_count * turn for turn in range(turns)]

    def spread(turn, origin, k):
        for bit in reversed(range(bits)):
            @pl.when(distances[turn] < (1 << bit))
            def _(bit=bit):
                tile_copy(turn, origin, k, bit + 1, False).start()
        tile_copy(turn, origin, k, 0, False).start()

    def direct(step):
        return bits == 2 and step == col_count - 1

    def far_copy(turn, origin, k):
        where = (origin, pieces[k][0], pieces[k][1])
        return pltpu.make_async_remote_copy(
            src_ref=own.at[where], dst_ref=cols.at[(turn,) + where],
            send_sem=f_send.at[k], recv_sem=c_recv.at[turn, origin, k],
            device_id={"row": flip(flip(row, 1), 2), "col": col}, device_id_type=MESH)

    def line_step(phase, step):
        @pl.when(origin_ok(phase, step))
        def _():
            origin = col - along(phase) * step
            for k in range(len(pieces)):
                if step > 0:
                    line_copy(phase, step, k).wait_recv()

                @pl.when(target_ok(phase))
                def _(k=k):
                    line_copy(phase, step, k).start()

                if phase == 0 or step > 0:
                    @pl.when(at_home)
                    def _(k=k):
                        if direct(step):
                            far_copy(home_turn, origin, k).start()
                        for bit in reversed(range(bits + 1)):
                            tile_copy(home_turn, origin, k, bit, True).start()

    relays = [carrier & away[turn] & (distances[turn] < (1 << (bits - 1))) for turn in range(turns)]
    leaves = [carrier & (distances[turn] >= (1 << (bits - 1))) for turn in range(turns)]

    def tile_step(phase, step, roles):
        @pl.when(origin_ok(phase, step))
        def _():
            origin = col - along(phase) * step
            for k in range(len(pieces)):
                for turn in range(turns):
                    @pl.when(roles[turn])
                    def _(turn=turn, k=k):
                        tile_copy(turn, origin, k, 0, False).wait_recv()
                        if roles is relays and not direct(step):
                            spread(turn, origin, k)
                        else:
                            tile_copy(turn, origin, k, 0, False).start()

    def line_drain(phase):
        @pl.when(target_ok(phase))
        def _():
            for step in range(col_count):
                @pl.when(origin_ok(phase, step))
                def _(step=step):
                    for k in range(len(pieces)):
                        line_copy(phase, step, k).wait_send()

    steps = [(0, 0)] + [(phase, step) for step in range(1, col_count) for phase in (0, 1)]
    for place in range(len(steps) + LEAF_LAG):
        if place < len(steps):
            line_step(*steps[place])
            if steps[place] == (0, 0):
                line_step(1, 0)
        if 0 <= place - RELAY_LAG < len(steps):
            tile_step(*steps[place - RELAY_LAG], relays)
        if 0 <= place - LEAF_LAG < len(steps):
            tile_step(*steps[place - LEAF_LAG], leaves)

    line_drain(0)
    line_drain(1)

    depth = panels * width

    def fill(target, block, places):
        for origin in range(col_count):
            for p in range(panels):
                value = block[origin, p]
                high = value.astype(jnp.bfloat16)
                low = (value - high.astype(jnp.float32)).astype(jnp.bfloat16)
                for place, half in enumerate(places):
                    target[pl.ds(origin * height, height), pl.ds(place * depth + p * width, width)] = (
                        high if half == 0 else low)

    fill(left, own, (0, 0, 1))
    for turn in range(turns):
        @pl.when(col + col_count * turn > row)
        def _(turn=turn):
            out[turn] = jnp.zeros(out.shape[1:], jnp.float32)

    def each_origin(origin, carry):
        for turn in range(turns):
            for k in range(len(pieces)):
                @pl.when(carrier)
                def _(turn=turn, k=k):
                    for bit in range(bits):
                        passes = distances[turn] < (1 << bit)
                        if bits == 2:
                            far = (origin - col == col_count - 1) | (col - origin == col_count - 1)
                            passes = passes & (jnp.logical_not(far) | (distances[turn] == 0))

                        @pl.when(passes)
                        def _(bit=bit):
                            tile_copy(turn, origin, k, bit + 1, False).wait_send()
                    tile_copy(turn, origin, k, 0, False).wait_send()

                @pl.when(jnp.logical_not(carrier))
                def _(turn=turn, k=k):
                    tile_copy(turn, origin, k, 0, False).wait_recv()
        return carry

    lax.fori_loop(0, col_count, each_origin, 0)
    if bits == 2:
        @pl.when(at_home & ((col == 0) | (col == col_count - 1)))
        def _():
            for k in range(len(pieces)):
                far_copy(home_turn, col_count - 1 - col, k).wait_send()


    for turn in range(turns):
        tile = col + col_count * turn

        @pl.when(tile <= row)
        def _(turn=turn):
            @pl.when(jnp.logical_not(away[turn]))
            def _():
                fill(right, own, (0, 1, 0))

            @pl.when(away[turn])
            def _():
                fill(right, cols.at[turn], (0, 1, 0))

            out[turn] = lax.dot_general(left[...], right[...], (((1,), (1,)), ((), ())),
                                        preferred_element_type=jnp.float32)


def body(jacobian):
    row_count = lax.axis_size("row")
    col_count = lax.axis_size("col")
    turns = row_count // col_count
    panels, height, width = jacobian.shape
    tile = height * col_count
    pieces = panels * SPLIT
    bits = (row_count // 2).bit_length() - 1
    dma = pltpu.SemaphoreType.DMA
    blocks = pl.pallas_call(
        functools.partial(kernel, row_count, col_count),
        out_shape=jax.ShapeDtypeStruct((turns, tile, tile), jnp.float32),
        in_specs=[pl.BlockSpec(memory_space=pl.ANY)],
        out_specs=pl.BlockSpec(memory_space=pltpu.VMEM),
        scratch_shapes=[
            pltpu.VMEM((col_count, panels, height, width), jnp.float32),
            pltpu.VMEM((turns, col_count, panels, height, width), jnp.float32),
            pltpu.VMEM((tile, 3 * panels * width), jnp.bfloat16),
            pltpu.VMEM((tile, 3 * panels * width), jnp.bfloat16),
            dma,
            dma((2, col_count, pieces)),
            dma((col_count, pieces)),
            dma((turns, col_count, pieces, bits + 1)),
            dma((turns, col_count, pieces)),
            dma((pieces,)),
        ],
        compiler_params=pltpu.CompilerParams(collective_id=0, has_side_effects=True),
    )(jacobian)
    return blocks[None, :, None]


def solution(mesh):
    in_specs = (P(None, ("row", "col"), None),)
    out_specs = P("row", None, "col", None, None)
    return jax.shard_map(body, mesh=mesh, in_specs=in_specs, out_specs=out_specs, check_vma=False)
```
